128 devices in a mesh: ma: 64 (over x_hi, y, z, core), row: 2 (over x_lo).
Axes of the slice: x: 4 (x_hi: 2, x_lo: 2; x = x_hi * 2 + x_lo), y: 4, z: 4, core: 2. Of those that a mesh axis runs over, the one named last changes fastest.
Arguments:
- spectral: bfloat16 [384, 2, 384, 2, 769], P('ma', None, 'row'), may hold values from -0.011047363 to 0.011047363
- latitude_basis: bfloat16 [384, 769, 1152], P('ma'), may hold values from -0.21875 to 0.21875
- pair_orders: int32 [384], replicated, may hold values from 0 to 383, each once
Outputs:
- grid_values: bfloat16 [64, 2, 1152, 2304], P('row', None, 'ma')
The draws below stay inside these ranges and needn't reach their ends.
Inputs may be any that keep to these rules, and one draw needn't show every extreme that they name: A permutation of 0 to 383; slot p holds the orders pair_orders[p] and 767 - pair_orders[p].
All inputs are finite; a program needn't handle non-finite values.
Results may differ from the reference program's by a relative error of at most 0.0066.
Values may be sent and summed in bfloat16 or wider, within the bound.
A program may use at most 128 MiB of HBM per device.

```python
import math
import jax
import jax.numpy as jnp
from jax import lax

L = 768
NCHEB = 384
NLAT = 1152
NLON = 2304
FIELDS = 2
LEV = 64
PAIRS = 384
PACKED = 769


def shard_levels(stream_key, dims, shards, smallest, largest):
    def one(axis_at, blocks):
        heights = jax.random.uniform(jax.random.fold_in(jax.random.fold_in(stream_key, 6), axis_at), (blocks,), jnp.float32, smallest / len(shards), largest / len(shards))
        return jnp.repeat(jnp.exp(heights), dims[axis_at] // blocks).reshape((-1,) + (1,) * (len(dims) - axis_at - 1))

    gain = one(*shards[0])
    for cut in shards[1:]:
        gain = gain * one(*cut)
    return gain


def normal_values(rng, extent, width, reach, cuts=(), held_as=jnp.bfloat16):
    factor_of = shard_levels(rng, extent, cuts, -0.22, 0.18) if cuts else 1.0
    array = jax.random.normal(rng, extent, jnp.float32) * width * factor_of
    return jnp.minimum(jnp.maximum(array, -reach), reach).astype(held_as)


def setup_inputs(seed: int = 0) -> dict:
    key_list = jax.random.split(jax.random.key(seed), 4)
    spectral = normal_values(key_list[0], (PAIRS, 2, NCHEB, FIELDS, PACKED), (1.0 / (NCHEB * L) ** 0.5), 0.011047363, ((0, 64), (2, 2)))
    latitude_basis = normal_values(key_list[1], (PAIRS, PACKED, NLAT), PACKED ** -0.5, 0.21875, ((0, 64),))
    pair_orders = jax.random.permutation(key_list[2], PAIRS).astype(jnp.int32)
    return dict(spectral=spectral, latitude_basis=latitude_basis, pair_orders=pair_orders)


def radial_table(total_modes, levels):
    mode_index = lax.broadcasted_iota(jnp.int32, (total_modes, levels), 0)
    points = lax.broadcasted_iota(jnp.int32, (total_modes, levels), 1)
    period = 2 * (total_modes - 1)
    phase_steps = (mode_index * points) % period
    return jnp.cos(phase_steps.astype(jnp.float32) * (2.0 * math.pi / period)).astype(jnp.bfloat16)


def longitude_table(pair_orders, degrees, points):
    lower_orders = pair_orders.astype(jnp.int32)
    orders = jnp.stack([lower_orders, degrees - 1 - lower_orders], axis=1)
    weights = jnp.where(orders == 0, 1.0, 2.0).astype(jnp.float32)
    phase_index = (orders[:, :, None] * lax.broadcasted_iota(jnp.int32, (1, 1, points), 2)) % points
    angles = phase_index.astype(jnp.float32) * (2.0 * math.pi / points)
    real_part = weights[:, :, None] * jnp.cos(angles)
    imag_part = -weights[:, :, None] * jnp.sin(angles)
    stacked = jnp.stack([real_part, imag_part], axis=2)
    return stacked.reshape(-1, points).astype(jnp.bfloat16)


def reference(spectral, latitude_basis, pair_orders):
    cheb_table = radial_table(NCHEB, LEV).astype(jnp.float32)
    lon_table = longitude_table(pair_orders, L, NLON).astype(jnp.float32)
    packed_rows = jnp.arange(PACKED, dtype=jnp.int32)

    def one_pair(pair_index):
        coeffs = lax.dynamic_index_in_dim(spectral, pair_index, 0, keepdims=False)
        basis_rows = lax.dynamic_index_in_dim(latitude_basis, pair_index, 0, keepdims=False)
        lower_order = lax.dynamic_index_in_dim(pair_orders, pair_index, 0, keepdims=False).astype(jnp.int32)
        below_split = packed_rows < (L - lower_order)
        selectors = jnp.stack([below_split, jnp.logical_not(below_split)], axis=0).astype(jnp.float32)
        summed = jnp.einsum("ckfr,kl->lfcr", coeffs.astype(jnp.float32), cheb_table)
        levels = lax.optimization_barrier(summed.astype(jnp.bfloat16)).astype(jnp.float32)
        masked = levels[None] * selectors[:, None, None, None, :]
        fourier = jnp.einsum("hlfcr,rt->lfhct", masked, basis_rows.astype(jnp.float32))
        return fourier.astype(jnp.bfloat16)

    fourier_all = lax.map(one_pair, jnp.arange(PAIRS, dtype=jnp.int32))
    stacked = jnp.transpose(fourier_all, (1, 2, 5, 0, 3, 4)).reshape(LEV, FIELDS, NLAT, PAIRS * 4)

    def one_level(level_block):
        return jnp.einsum("fto,on->ftn", level_block.astype(jnp.float32), lon_table).astype(jnp.bfloat16)

    return lax.map(one_level, stacked)
```

```python
import functools
import math

import jax
import jax.numpy as jnp
from jax import lax
from jax.experimental import pallas as pl
from jax.experimental.pallas import tpu as pltpu
from jax.sharding import PartitionSpec as P

NLON = 2304
LEV = 64
MESH = pl.DeviceIdType.MESH
BF = jnp.bfloat16
F32 = jnp.float32

GROUP = 64
STRIDE = 37
PAIR_DEV = 6
LANES = 128
TDEV = 18
NJ = 6
DEG = 768


def partner(ma, row, k):
    d = lax.rem(ma + lax.rem(k * STRIDE, GROUP), GROUP)
    half = GROUP // 2
    return d, lax.rem(row + ma // half + d // half, 2)


def kernel(
    spec, basis, last, table, cuts, rot_cos, rot_sin, fine_cos, fine_sin, out,
    stage, bas, own, got, lhs, sendbuf, recvbuf, lon, rx, acc, mix, grid,
    spec_sem, bas_sem, pair_send, pair_recv, send_sem, recv_sem, local_sem, out_sem,
):
    ma = lax.axis_index("ma")
    row = lax.axis_index("row")
    side = lax.rem(row + ma // (GROUP // 2), 2)

    def load_spec(p, j):
        return pltpu.make_async_copy(
            spec.at[p, :, :, :, pl.ds(j * LANES, LANES)], stage.at[p, j], spec_sem.at[p, j]
        )

    def load_basis(p):
        return pltpu.make_async_copy(basis.at[p], bas.at[p], bas_sem.at[p])

    for p in range(PAIR_DEV):
        for j in range(NJ):
            load_spec(p, j).start()
    for p in range(PAIR_DEV):
        load_basis(p).start()

    barrier = pltpu.get_barrier_semaphore()
    pl.semaphore_signal(barrier, inc=1, device_id=(ma, 1 - row), device_id_type=MESH)

    def greet(k, carry):
        pl.semaphore_signal(barrier, inc=1, device_id=partner(ma, row, k), device_id_type=MESH)
        return carry

    lax.fori_loop(1, GROUP, greet, 0)

    def pair_copy(p):
        return pltpu.make_async_remote_copy(
            src_ref=own.at[p],
            dst_ref=got.at[p],
            send_sem=pair_send.at[p],
            recv_sem=pair_recv.at[p],
            device_id=(ma, 1 - row),
            device_id_type=MESH,
        )

    def radial(p):
        for j in range(NJ):
            load_spec(p, j).wait()
            for c in range(2):
                modes = stage[p, j, c].reshape(2 * 192, LANES)
                part = jnp.dot(table[...], modes, preferred_element_type=F32).astype(BF)
                own[p, pl.ds(128 * j + 32 * c, 32)] = part[:64].reshape(32, 2, LANES)
                own[p, pl.ds(128 * j + 64 + 32 * c, 32)] = part[64:].reshape(32, 2, LANES)
        own[p, 768] = last[p]

    radial(0)
    pl.semaphore_wait(barrier, GROUP)
    pair_copy(0).start()

    def more(p, carry):
        radial(p)
        pair_copy(p).start()
        return carry

    lax.fori_loop(1, PAIR_DEV, more, 0)

    def clear(i, carry):
        acc[pl.ds(i * 64, 64), :] = jnp.zeros((64, NLON), F32)
        return carry

    lax.fori_loop(0, TDEV, clear, 0)

    def longitude(q):
        cos_b, sin_b = fine_cos[q], fine_sin[q]
        rc, rs = rot_cos[q], rot_sin[q]
        for i in range(NLON // LANES):
            cos_a, sin_a = rc[:, i : i + 1], rs[:, i : i + 1]
            cols = pl.ds(i * LANES, LANES)
            lon[pl.ds(0, 128), cols] = (cos_a * cos_b - sin_a * sin_b).astype(BF)
            lon[pl.ds(128, 128), cols] = (-(sin_a * cos_b + cos_a * sin_b)).astype(BF)

    def latitude(q):
        pair_copy(q).wait_recv()
        cut = cuts[q]
        for j in range(NJ):
            rows = pl.ds(128 * j, 128)
            levels = (
                own[q, rows].reshape(256, LANES).astype(F32)
                + got[q, rows].reshape(256, LANES).astype(F32)
            ).astype(BF).astype(F32)
            low = lax.broadcasted_iota(jnp.int32, (256, LANES), 1) + 128 * j < cut
            below = jnp.where(low, levels, 0.0).astype(BF)
            above = jnp.where(low, 0.0, levels).astype(BF)
            for half in range(2):
                lhs[half, pl.ds(0, 128), pl.ds(128 * j, 128)] = below[128 * half : 128 * half + 128]
                lhs[half, pl.ds(128, 128), pl.ds(128 * j, 128)] = above[128 * half : 128 * half + 128]
        tail = (own[q, 768].astype(F32) + got[q, 768].astype(F32)).astype(BF).astype(F32)
        load_basis(q).wait()
        first = lax.broadcasted_iota(jnp.int32, (1, LANES), 1) * 0 + side == 0
        tails = (
            jnp.where(first, tail[0:1], tail[1:2]),
            jnp.where(first, tail[1:2], tail[0:1]),
        )

        def block(t0, which, lo, hi):
            half = side if which == 0 else 1 - side
            cols = pl.ds(t0, 128)
            got_t = lax.dot_general(
                bas[q, pl.ds(0, DEG), cols],
                lhs[half],
                (((0,), (1,)), ((), ())),
                preferred_element_type=F32,
            )
            edge = jnp.transpose(bas[q, pl.ds(DEG, 1), cols].astype(F32), (1, 0))
            mix[pl.ds(0, 128, 2), :] = got_t[:, :128]
            mix[pl.ds(1, 128, 2), :] = got_t[:, 128:] + edge * tails[which]
            sendbuf[q, pl.ds(t0 + lo, hi - lo)] = (
                mix[pl.ds(2 * lo, 2 * (hi - lo)), :].astype(BF).reshape(hi - lo, 2, LANES)
            )

        for b in range(4):
            block(128 * b, 0, 0, 128)
        block(512, 0, 0, 64)
        block(512, 1, 64, 128)
        for b in range(5, 9):
            block(128 * b, 1, 0, 128)

    def scatter_copy(q, k):
        d, r = partner(ma, row, k)
        return pltpu.make_async_remote_copy(
            src_ref=sendbuf.at[q, pl.ds(TDEV * d, TDEV)],
            dst_ref=recvbuf.at[q, :, ma],
            send_sem=send_sem.at[q],
            recv_sem=recv_sem.at[q],
            device_id=(d, r),
            device_id_type=MESH,
        )

    def scatter(q):
        def send(k, carry):
            scatter_copy(q, k).start()
            return carry

        lax.fori_loop(1, GROUP, send, 0)
        pltpu.make_async_copy(
            sendbuf.at[q, pl.ds(TDEV * ma, TDEV)], recvbuf.at[q, :, ma], local_sem.at[q]
        ).start()

    def arrive(q):
        pltpu.make_async_copy(
            sendbuf.at[q, pl.ds(TDEV * ma, TDEV)], recvbuf.at[q, :, ma], local_sem.at[q]
        ).wait()
        pltpu.make_async_copy(
            recvbuf.at[q, :, pl.ds(0, GROUP - 1)],
            recvbuf.at[q, :, pl.ds(0, GROUP - 1)],
            recv_sem.at[q],
        ).wait()
        for t in range(TDEV):
            turned = recvbuf[q, t].reshape(128, LANES).T
            rx[pl.ds(64 * t, 64), pl.ds(0, 128)] = turned[:64]
            rx[pl.ds(64 * t, 64), pl.ds(128, 128)] = turned[64:]

    def receive(q):
        longitude(q)
        arrive(q)
        for g in range(3):
            rows = pl.ds(384 * g, 384)
            left = rx[rows, :]
            for n in range(9):
                cols = pl.ds(256 * n, 256)
                acc[rows, cols] += jnp.dot(left, lon[:, cols], preferred_element_type=F32)

    latitude(0)
    scatter(0)

    def step(q, carry):
        latitude(q)
        scatter(q)
        receive(q - 1)
        return carry

    lax.fori_loop(1, PAIR_DEV, step, 0)

    end = PAIR_DEV - 1
    longitude(end)
    arrive(end)

    def put(t, n):
        return pltpu.make_async_copy(
            grid.at[t, n], out.at[:, t, :, pl.ds(n * LANES, LANES)], out_sem
        )

    for g in range(9):
        rows = pl.ds(128 * g, 128)
        left = rx[rows, :]
        for n in range(9):
            cols = pl.ds(256 * n, 256)
            total = (
                acc[rows, cols] + jnp.dot(left, lon[:, cols], preferred_element_type=F32)
            ).astype(BF)
            for a in range(2):
                for b in range(2):
                    grid[2 * g + a, 2 * n + b] = total[
                        64 * a : 64 * a + 64, 128 * b : 128 * b + 128
                    ].reshape(32, 2, LANES)
        for a in range(2):
            for n in range(18):
                put(2 * g + a, n).start()

    def drain(q, carry):
        pair_copy(q).wait_send()
        pltpu.make_async_copy(
            sendbuf.at[q, pl.ds(0, TDEV * (GROUP - 1))],
            sendbuf.at[q, pl.ds(0, TDEV * (GROUP - 1))],
            send_sem.at[q],
        ).wait()
        return carry

    lax.fori_loop(0, PAIR_DEV, drain, 0)
    pltpu.make_async_copy(grid, grid, out_sem).wait()


def radial_table(total_modes, levels):
    mode_index = lax.broadcasted_iota(jnp.int32, (total_modes, levels), 0)
    points = lax.broadcasted_iota(jnp.int32, (total_modes, levels), 1)
    period = 2 * (total_modes - 1)
    phase_steps = mode_index * points % period
    return jnp.cos(phase_steps.astype(F32) * (2.0 * math.pi / period)).astype(BF)


def angles_of(orders, steps):
    return (orders * steps % NLON).astype(F32) * (2.0 * math.pi / NLON)


def per_device(spectral, latitude_basis, pair_orders):
    pair_dev, parts, local_modes, fields, packed = spectral.shape
    degrees = packed - 1
    row_count = lax.axis_size("row")
    level_dev = LEV // row_count
    cheb = lax.dynamic_slice_in_dim(
        radial_table(local_modes * row_count, LEV), lax.axis_index("row") * local_modes, local_modes, 0
    )
    eye = jnp.eye(fields, dtype=BF)
    table = (cheb.T[:, None, :, None] * eye[None, :, None, :]).reshape(
        LEV * fields, local_modes * fields
    )
    last = jnp.einsum(
        "pckf,kl->pclf", spectral[..., degrees], cheb, preferred_element_type=F32
    ).astype(BF)
    last = last.reshape(pair_dev, parts, row_count, level_dev * fields)
    last = jnp.transpose(last, (0, 2, 1, 3)).reshape(pair_dev, row_count, LANES)
    local_orders = lax.dynamic_slice_in_dim(
        pair_orders, lax.axis_index("ma") * pair_dev, pair_dev, 0
    )
    cuts = degrees - local_orders
    orders = jnp.stack([pair_orders, degrees - 1 - pair_orders], axis=1)
    orders = jnp.transpose(orders.reshape(GROUP, pair_dev, 2), (1, 0, 2)).reshape(
        pair_dev, GROUP * 2, 1
    )
    lanes = lax.broadcasted_iota(jnp.int32, (1, 1, LANES), 2)
    weights = jnp.where(orders == 0, 1.0, 2.0).astype(F32)
    coarse = angles_of(orders, lanes[..., : NLON // LANES] * LANES)
    fine = angles_of(orders, lanes)
    result = pl.pallas_call(
        kernel,
        out_shape=jax.ShapeDtypeStruct((level_dev, TDEV, fields, NLON), BF),
        in_specs=[
            pl.BlockSpec(memory_space=pl.ANY),
            pl.BlockSpec(memory_space=pl.ANY),
            pl.BlockSpec(memory_space=pltpu.VMEM),
            pl.BlockSpec(memory_space=pltpu.VMEM),
            pl.BlockSpec(memory_space=pltpu.SMEM),
        ]
        + [pl.BlockSpec(memory_space=pltpu.VMEM)] * 4,
        out_specs=pl.BlockSpec(memory_space=pl.ANY),
        scratch_shapes=[
            pltpu.VMEM((pair_dev, NJ, parts, local_modes, fields, LANES), BF),
            pltpu.VMEM((pair_dev, packed, 1152), BF),
            pltpu.VMEM((pair_dev, packed, 2, LANES), BF),
            pltpu.VMEM((pair_dev, packed, 2, LANES), BF),
            pltpu.VMEM((2, 256, degrees), BF),
            pltpu.VMEM((pair_dev, 1152, 2, LANES), BF),
            pltpu.VMEM((pair_dev, TDEV, GROUP, 2, LANES), BF),
            pltpu.VMEM((256, NLON), BF),
            pltpu.VMEM((1152, 256), BF),
            pltpu.VMEM((1152, NLON), F32),
            pltpu.VMEM((256, LANES), F32),
            pltpu.VMEM((TDEV, NLON // LANES, level_dev, fields, LANES), BF),
            pltpu.SemaphoreType.DMA((pair_dev, NJ)),
            pltpu.SemaphoreType.DMA((pair_dev,)),
            pltpu.SemaphoreType.DMA((pair_dev,)),
            pltpu.SemaphoreType.DMA((pair_dev,)),
            pltpu.SemaphoreType.DMA((pair_dev,)),
            pltpu.SemaphoreType.DMA((pair_dev,)),
            pltpu.SemaphoreType.DMA((pair_dev,)),
            pltpu.SemaphoreType.DMA,
        ],
        compiler_params=pltpu.CompilerParams(
            collective_id=0, has_side_effects=True, vmem_limit_bytes=66_000_000
        ),
    )(
        spectral,
        latitude_basis,
        last,
        table,
        cuts,
        weights * jnp.cos(coarse),
        weights * jnp.sin(coarse),
        jnp.cos(fine),
        jnp.sin(fine),
    )
    return jnp.transpose(result, (0, 2, 1, 3))


def solution(mesh):
    return jax.shard_map(
        per_device,
        mesh=mesh,
        in_specs=(P("ma", None, "row", None, None), P("ma", None, None), P()),
        out_specs=P("row", None, "ma", None),
        check_vma=False,
    )
```

```python
import functools
import math

import jax
import jax.numpy as jnp
from jax import lax
from jax.experimental import pallas as pl
from jax.experimental.pallas import tpu as pltpu
from jax.sharding import PartitionSpec as P

NLON = 2304
LEV = 64
MESH = pl.DeviceIdType.MESH
BF = jnp.bfloat16
F32 = jnp.float32

PLANE = 32
STRIDE = 13
PAIR_DEV = 6
LANES = 128
TDEV = 18
NJ = 6
DEG = 768
MODES = 192
TURN = 2.0 * math.pi


def cosine(steps, period):
    left = steps - period * jnp.floor(steps * (1.0 / period) + 0.5)
    size = jnp.abs(left)
    flip = size > period / 4
    angle = jnp.where(flip, period / 2 - size, size) * (TURN / period)
    square = angle * angle
    total = jnp.full_like(square, -1.0 / math.factorial(14))
    for n in range(12, -1, -2):
        total = total * square + (-1.0) ** (n // 2) / math.factorial(n)
    return jnp.where(flip, -total, total)


def kernel(
    spec, basis, orders_row, orders, out,
    stage, rows, bas, own, got, lhs, sendbuf, recvbuf, lon, rx, acc, mix, table, grid,
    spec_sem, rows_sem, bas_sem, pair_send, pair_recv, send_sem, recv_sem, meet, out_sem,
):
    ma = lax.axis_index("ma")
    row = lax.axis_index("row")
    plane = ma // PLANE
    place = lax.rem(ma, PLANE)
    along_y, along_z, core = place // 8, lax.rem(place // 2, 4), lax.rem(place, 2)

    def load_spec(p, j):
        return pltpu.make_async_copy(
            spec.at[p, :, :, :, pl.ds(j * LANES, LANES)], stage.at[p, j], spec_sem.at[p, j]
        )

    def load_rows(p):
        slot = lax.rem(p, 2)
        return pltpu.make_async_copy(spec.at[p], rows.at[slot], rows_sem.at[slot])

    def load_basis(p):
        return pltpu.make_async_copy(basis.at[p], bas.at[p], bas_sem.at[p])

    for p in range(PAIR_DEV):
        for j in range(NJ):
            load_spec(p, j).start()
        if p < 2:
            load_rows(p).start()
        else:
            load_basis(p - 2).start()
    for p in range(PAIR_DEV - 2, PAIR_DEV):
        load_basis(p).start()

    def signal(sem, device):
        pl.semaphore_signal(sem, inc=1, device_id=device, device_id_type=MESH)

    def on_y(i):
        return plane * PLANE + lax.rem(along_y + i, 4) * 8 + along_z * 2 + core, row

    def on_z(i):
        return plane * PLANE + along_y * 8 + lax.rem(along_z + i, 4) * 2 + core, row

    across = ((1 - plane) * PLANE + place, 1 - row)
    barrier = pltpu.get_barrier_semaphore()
    signal(barrier, (ma, 1 - row))
    for i in range(1, 4):
        signal(barrier, on_y(i))
    for i in range(1, 4):
        signal(barrier, on_z(i))
    signal(barrier, (plane * PLANE + along_y * 8 + along_z * 2 + 1 - core, row))
    signal(barrier, across)

    level = lax.broadcasted_iota(jnp.int32, (LANES, 2 * MODES), 0)
    mode = lax.broadcasted_iota(jnp.int32, (LANES, 2 * MODES), 1)
    steps = (level // 2) * (mode // 2 + row * MODES)
    same = lax.rem(level, 2) == lax.rem(mode, 2)
    period = 2 * (2 * MODES - 1)
    table[...] = jnp.where(same, cosine(steps.astype(F32), period), 0.0).astype(BF)

    def pair_copy(p, w):
        half = row if w == 0 else 1 - row
        return pltpu.make_async_remote_copy(
            src_ref=own.at[p, half],
            dst_ref=got.at[p, half],
            send_sem=pair_send.at[p, w],
            recv_sem=pair_recv.at[p, w],
            device_id=(ma, 1 - row),
            device_id_type=MESH,
        )

    def radial(p):
        ends = []
        for j in range(NJ):
            load_spec(p, j).wait()
            for c in range(2):
                modes = stage[p, j, c].reshape(2 * MODES, LANES)
                part = jnp.dot(table[...], modes, preferred_element_type=F32).astype(BF)
                for half in range(2):
                    own[p, half, pl.ds(64 * j + 32 * c, 32)] = part[
                        64 * half : 64 * half + 64
                    ].reshape(32, 2, LANES)
        load_rows(p).wait()
        for c in range(2):
            modes = rows[lax.rem(p, 2), c, :, :, DEG : DEG + 1].reshape(2 * MODES, 1)
            ends.append(
                lax.dot_general(
                    modes, table[...], (((0,), (1,)), ((), ())), preferred_element_type=F32
                )
            )
        for half in range(2):
            joined = jnp.concatenate([e[:, 64 * half : 64 * half + 64] for e in ends], axis=1)
            own[p, half, 64 * NJ] = jnp.broadcast_to(joined.astype(BF), (2, LANES))

    def more(p):
        radial(p)
        pair_copy(p, 0).start()
        pair_copy(p, 1).start()

    def longitude(q):
        k = lax.broadcasted_iota(jnp.int32, (LANES, PLANE * 2 * PAIR_DEV), 0)
        slot = lax.broadcasted_iota(jnp.int32, (LANES, PLANE * 2 * PAIR_DEV), 1)
        picked = jnp.where(slot == (k // 2) * PAIR_DEV + q, orders_row[...].reshape(1, PLANE * 2 * PAIR_DEV).astype(F32), 0.0)
        lower = jnp.sum(picked, axis=1, keepdims=True)
        odd = lax.rem(lax.broadcasted_iota(jnp.int32, (LANES, 1), 0), 2) == 1
        order = jnp.where(odd, DEG - 1 - lower, lower)
        weight = jnp.where(order == 0, 1.0, 2.0)
        lane = lax.broadcasted_iota(jnp.int32, (LANES, LANES), 1).astype(F32)
        fine = order * lane
        cos_b, sin_b = cosine(fine, NLON), cosine(fine - NLON // 4, NLON)
        coarse = order * jnp.where(lane < NLON // LANES, lane, 0.0) * LANES
        cos_all = weight * cosine(coarse, NLON)
        sin_all = weight * cosine(coarse - NLON // 4, NLON)
        for i in range(NLON // LANES):
            cos_a, sin_a = cos_all[:, i : i + 1], sin_all[:, i : i + 1]
            cols = pl.ds(i * LANES, LANES)
            lon[pl.ds(0, 128), cols] = (cos_a * cos_b - sin_a * sin_b).astype(BF)
            lon[pl.ds(128, 128), cols] = (-(sin_a * cos_b + cos_a * sin_b)).astype(BF)

    def latitude(q, w):
        half = 1 - row if w == 0 else row
        to = 1 - plane if w == 0 else plane
        pair_copy(q, w).wait_recv()
        cut = DEG - orders[ma * PAIR_DEV + q]
        for j in range(NJ):
            piece = pl.ds(64 * j, 64)
            levels = (
                own[q, half, piece].reshape(128, LANES).astype(F32)
                + got[q, half, piece].reshape(128, LANES).astype(F32)
            )
            low = lax.broadcasted_iota(jnp.int32, (128, LANES), 1) + 128 * j < cut
            lhs[w, pl.ds(0, 128), pl.ds(128 * j, 128)] = jnp.where(low, levels, 0.0).astype(BF)
            lhs[w, pl.ds(128, 128), pl.ds(128 * j, 128)] = jnp.where(low, 0.0, levels).astype(BF)
        end = own[q, half, 64 * NJ].astype(F32) + got[q, half, 64 * NJ].astype(F32)
        end = end.astype(BF).astype(F32)[0:1]
        if w == 0:
            load_basis(q).wait()
        for b in range(5):
            cols = pl.ds(pl.multiple_of(to * 512 + 128 * b, 128), 128)
            made = lax.dot_general(
                bas[q, pl.ds(0, DEG), cols],
                lhs[w],
                (((0,), (1,)), ((), ())),
                preferred_element_type=F32,
            )
            edge = jnp.transpose(bas[q, pl.ds(DEG, 1), cols].astype(F32), (1, 0))
            mix[b % 2, pl.ds(0, 128, 2), :] = made[:, :128]
            mix[b % 2, pl.ds(1, 128, 2), :] = made[:, 128:] + edge * end
            sendbuf[q, w, pl.ds(128 * b, 128)] = mix[b % 2].astype(BF).reshape(128, 2, LANES)

    def scatter_copy(q, w, k):
        to = 1 - plane if w == 0 else plane
        other = lax.rem(place + lax.rem(k * STRIDE, PLANE), PLANE)
        return pltpu.make_async_remote_copy(
            src_ref=sendbuf.at[q, w, pl.ds(64 * to + TDEV * other, TDEV)],
            dst_ref=recvbuf.at[q, :, ma],
            send_sem=send_sem.at[q, w],
            recv_sem=recv_sem.at[q, w],
            device_id=(to * PLANE + other, 1 - row if w == 0 else row),
            device_id_type=MESH,
        )

    def scatter_across(q):
        def send(k, carry):
            scatter_copy(q, 0, k).start()
            return carry

        lax.fori_loop(0, PLANE, send, 0, unroll=4)

    def keep(q):
        return pltpu.make_async_copy(
            sendbuf.at[q, 1, pl.ds(64 * plane + TDEV * place, TDEV)],
            recvbuf.at[q, :, ma],
            recv_sem.at[q, 1],
        )

    def scatter_inside(q):
        def send(k, carry):
            scatter_copy(q, 1, k).start()
            return carry

        lax.fori_loop(1, PLANE, send, 0, unroll=4)
        keep(q).start()

    def scatter_both(q):
        scatter_copy(q, 0, 0).start()

        def send(k, carry):
            scatter_copy(q - 1, 1, k).start()
            scatter_copy(q, 0, k).start()
            return carry

        lax.fori_loop(1, PLANE, send, 0, unroll=2)
        keep(q - 1).start()

    def arrive(q):
        for w in range(2):
            arrived = recvbuf.at[q, :, pl.ds((1 - plane if w == 0 else plane) * PLANE, PLANE)]
            pltpu.make_async_copy(arrived, arrived, recv_sem.at[q, w]).wait()
        for t in range(TDEV):
            turned = recvbuf[q, t].reshape(128, LANES).T
            rx[pl.ds(64 * t, 64), pl.ds(0, 128)] = turned[:64]
            rx[pl.ds(64 * t, 64), pl.ds(128, 128)] = turned[64:]

    def receive(q, first=False):
        arrive(q)
        for g in range(3):
            part = pl.ds(384 * g, 384)
            left = rx[part, :]
            for n in range(9):
                cols = pl.ds(256 * n, 256)
                added = jnp.dot(left, lon[:, cols], preferred_element_type=F32)
                acc[part, cols] = added if first else acc[part, cols] + added

    radial(0)
    pl.semaphore_wait(barrier, 9)
    pair_copy(0, 0).start()
    pair_copy(0, 1).start()
    load_rows(2).start()
    for i in range(1, 4):
        signal(meet.at[0], on_y(i))
    more(1)
    load_rows(3).start()
    pl.semaphore_wait(meet.at[0], 3)
    for i in range(1, 4):
        signal(meet.at[1], on_z(i))
    longitude(0)
    pl.semaphore_wait(meet.at[1], 3)
    signal(meet.at[2], across)
    latitude(0, 0)
    pl.semaphore_wait(meet.at[2], 1)
    scatter_across(0)
    more(2)
    load_rows(4).start()
    latitude(0, 1)
    latitude(1, 0)
    scatter_both(1)
    more(3)
    load_rows(5).start()
    latitude(1, 1)
    latitude(2, 0)
    scatter_both(2)
    more(4)
    receive(0, True)
    longitude(1)
    latitude(2, 1)

    def step(q, carry):
        latitude(q, 0)
        scatter_both(q)

        @pl.when(q < PAIR_DEV - 2)
        def _():
            more(q + 2)

        receive(q - 2)
        longitude(q - 1)
        latitude(q, 1)
        return carry

    lax.fori_loop(3, PAIR_DEV, step, 0)

    end = PAIR_DEV - 1
    scatter_inside(end)
    receive(end - 1)
    longitude(end)
    arrive(end)

    def put(t):
        return pltpu.make_async_copy(grid.at[t], out.at[:, t], out_sem.at[t])

    for g in range(9):
        part = pl.ds(128 * g, 128)
        left = rx[part, :]
        for n in range(9):
            cols = pl.ds(256 * n, 256)
            total = (
                acc[part, cols] + jnp.dot(left, lon[:, cols], preferred_element_type=F32)
            ).astype(BF)
            for a in range(2):
                for b in range(2):
                    grid[2 * g + a, :, :, pl.ds(256 * n + 128 * b, LANES)] = total[
                        64 * a : 64 * a + 64, 128 * b : 128 * b + 128
                    ].reshape(32, 2, LANES)
        for a in range(2):
            put(2 * g + a).start()

    def drain(q, carry):
        for w in range(2):
            pair_copy(q, w).wait_send()
            sent = sendbuf.at[q, w, pl.ds(0, TDEV * (PLANE - w))]
            pltpu.make_async_copy(sent, sent, send_sem.at[q, w]).wait()
        return carry

    lax.fori_loop(0, PAIR_DEV, drain, 0)
    for t in range(TDEV):
        put(t).wait()


def write_out(grid, out, hold, read_sem, write_sem):
    reads, writes = [], []
    for i in range(8):
        piece = pl.ds(4 * i, 4)
        reads.append(pltpu.make_async_copy(grid.at[piece], hold.at[i], read_sem.at[i]))
        writes.append(pltpu.make_async_copy(hold.at[i], out.at[piece], write_sem.at[i]))
    for copy in reads:
        copy.start()
    for read, write in zip(reads, writes):
        read.wait()
        write.start()
    for copy in writes:
        copy.wait()


def per_device(spectral, latitude_basis, pair_orders):
    pair_dev, parts, local_modes, fields, packed = spectral.shape
    degrees = packed - 1
    level_dev = LEV // lax.axis_size("row")
    shape = jax.ShapeDtypeStruct((level_dev, TDEV, fields, NLON), BF)
    grid = pl.pallas_call(
        kernel,
        out_shape=shape,
        in_specs=[
            pl.BlockSpec(memory_space=pl.ANY),
            pl.BlockSpec(memory_space=pl.ANY),
            pl.BlockSpec(memory_space=pltpu.VMEM),
            pl.BlockSpec(memory_space=pltpu.SMEM),
        ],
        out_specs=pl.BlockSpec(memory_space=pl.ANY),
        scratch_shapes=[
            pltpu.VMEM((pair_dev, NJ, parts, local_modes, fields, LANES), BF),
            pltpu.VMEM((2, parts, local_modes, fields, packed), BF),
            pltpu.VMEM((pair_dev, packed, 1152), BF),
            pltpu.VMEM((pair_dev, 2, 64 * NJ + 1, 2, LANES), BF),
            pltpu.VMEM((pair_dev, 2, 64 * NJ + 1, 2, LANES), BF),
            pltpu.VMEM((2, 256, degrees), BF),
            pltpu.VMEM((pair_dev, 2, 640, 2, LANES), BF),
            pltpu.VMEM((pair_dev, TDEV, 2 * PLANE, 2, LANES), BF),
            pltpu.VMEM((256, NLON), BF),
            pltpu.VMEM((1152, 256), BF),
            pltpu.VMEM((1152, NLON), F32),
            pltpu.VMEM((2, 256, LANES), F32),
            pltpu.VMEM((LANES, fields * local_modes), BF),
            pltpu.VMEM((TDEV, level_dev, fields, NLON), BF),
            pltpu.SemaphoreType.DMA((pair_dev, NJ)),
            pltpu.SemaphoreType.DMA((2,)),
            pltpu.SemaphoreType.DMA((pair_dev,)),
            pltpu.SemaphoreType.DMA((pair_dev, 2)),
            pltpu.SemaphoreType.DMA((pair_dev, 2)),
            pltpu.SemaphoreType.DMA((pair_dev, 2)),
            pltpu.SemaphoreType.DMA((pair_dev, 2)),
            pltpu.SemaphoreType.REGULAR((3,)),
            pltpu.SemaphoreType.DMA((TDEV,)),
        ],
        compiler_params=pltpu.CompilerParams(
            collective_id=0, has_side_effects=True, vmem_limit_bytes=60 * 2**20
        ),
    )(spectral, latitude_basis, pair_orders, pair_orders)
    result = pl.pallas_call(
        write_out,
        out_shape=shape,
        in_specs=[pl.BlockSpec(memory_space=pl.ANY)],
        out_specs=pl.BlockSpec(memory_space=pl.ANY),
        scratch_shapes=[
            pltpu.VMEM((8, level_dev // 8, TDEV, fields, NLON), BF),
            pltpu.SemaphoreType.DMA((8,)),
            pltpu.SemaphoreType.DMA((8,)),
        ],
        compiler_params=pltpu.CompilerParams(vmem_limit_bytes=63 * 2**20),
    )(grid)
    return jnp.transpose(result, (0, 2, 1, 3))


def solution(mesh):
    return jax.shard_map(
        per_device,
        mesh=mesh,
        in_specs=(P("ma", None, "row", None, None), P("ma", None, None), P()),
        out_specs=P("row", None, "ma", None),
        check_vma=False,
    )
```

```python
import functools
import math

import jax
import jax.numpy as jnp
from jax import lax
from jax.experimental import pallas as pl
from jax.experimental.pallas import tpu as pltpu
from jax.sharding import PartitionSpec as P

NLON = 2304
LEV = 64
MESH = pl.DeviceIdType.MESH
BF = jnp.bfloat16
F32 = jnp.float32

PLANE = 32
STRIDE = 5
PAIR_DEV = 6
LANES = 128
TDEV = 18
NJ = 6
DEG = 768
MODES = 192
TURN = 2.0 * math.pi


def cosine(steps, period):
    left = steps - period * jnp.floor(steps * (1.0 / period) + 0.5)
    size = jnp.abs(left)
    flip = size > period / 4
    angle = jnp.where(flip, period / 2 - size, size) * (TURN / period)
    square = angle * angle
    total = jnp.full_like(square, -1.0 / math.factorial(14))
    for n in range(12, -1, -2):
        total = total * square + (-1.0) ** (n // 2) / math.factorial(n)
    return jnp.where(flip, -total, total)


def kernel(
    spec, basis, orders_row, orders, out,
    stage, rows, bas, own, got, lhs, sendbuf, recvbuf, lon, rx, acc, mix, table, grid,
    spec_sem, rows_sem, bas_sem, pair_send, pair_recv, send_sem, recv_sem, meet, out_sem,
):
    ma = lax.axis_index("ma")
    row = lax.axis_index("row")
    plane = ma // PLANE
    place = lax.rem(ma, PLANE)
    along_y, along_z, core = place // 8, lax.rem(place // 2, 4), lax.rem(place, 2)

    def load_spec(p, j):
        return pltpu.make_async_copy(
            spec.at[p, :, :, :, pl.ds(j * LANES, LANES)], stage.at[p, j], spec_sem.at[p, j]
        )

    def load_rows(p):
        slot = lax.rem(p, 2)
        return pltpu.make_async_copy(spec.at[p], rows.at[slot], rows_sem.at[slot])

    def load_basis(p):
        return pltpu.make_async_copy(basis.at[p], bas.at[p], bas_sem.at[p])

    for j in range(NJ):
        load_spec(0, j).start()
    load_rows(0).start()

    def load_others():
        for p in range(1, PAIR_DEV):
            for j in range(NJ):
                load_spec(p, j).start()
            if p == 1:
                load_rows(1).start()
            else:
                load_basis(p - 2).start()
        for p in range(PAIR_DEV - 2, PAIR_DEV):
            load_basis(p).start()

    def signal(sem, device):
        pl.semaphore_signal(sem, inc=1, device_id=device, device_id_type=MESH)

    def on_y(i):
        return plane * PLANE + lax.rem(along_y + i, 4) * 8 + along_z * 2 + core, row

    def on_z(i):
        return plane * PLANE + along_y * 8 + lax.rem(along_z + i, 4) * 2 + core, row

    across = ((1 - plane) * PLANE + place, 1 - row)
    barrier = pltpu.get_barrier_semaphore()
    signal(barrier, (ma, 1 - row))
    for i in range(1, 4):
        signal(barrier, on_y(i))
    for i in range(1, 4):
        signal(barrier, on_z(i))
    signal(barrier, (plane * PLANE + along_y * 8 + along_z * 2 + 1 - core, row))
    signal(barrier, across)

    level = lax.broadcasted_iota(jnp.int32, (LANES, 2 * MODES), 0)
    mode = lax.broadcasted_iota(jnp.int32, (LANES, 2 * MODES), 1)
    steps = (level // 2) * (mode // 2 + row * MODES)
    same = lax.rem(level, 2) == lax.rem(mode, 2)
    period = 2 * (2 * MODES - 1)
    table[...] = jnp.where(same, cosine(steps.astype(F32), period), 0.0).astype(BF)

    def pair_copy(p, w):
        half = row if w == 0 else 1 - row
        return pltpu.make_async_remote_copy(
            src_ref=own.at[p, half],
            dst_ref=got.at[p, half],
            send_sem=pair_send.at[p, w],
            recv_sem=pair_recv.at[p, w],
            device_id=(ma, 1 - row),
            device_id_type=MESH,
        )

    def radial(p, first=False):
        ends = []
        for j in range(NJ):
            load_spec(p, j).wait()
            if first and j == NJ - 1:
                load_others()
            for c in range(2):
                modes = stage[p, j, c].reshape(2 * MODES, LANES)
                part = jnp.dot(table[...], modes, preferred_element_type=F32).astype(BF)
                for half in range(2):
                    own[p, half, pl.ds(64 * j + 32 * c, 32)] = part[
                        64 * half : 64 * half + 64
                    ].reshape(32, 2, LANES)
        load_rows(p).wait()
        for c in range(2):
            modes = rows[lax.rem(p, 2), c, :, :, DEG : DEG + 1].reshape(2 * MODES, 1)
            ends.append(
                lax.dot_general(
                    modes, table[...], (((0,), (1,)), ((), ())), preferred_element_type=F32
                )
            )
        for half in range(2):
            joined = jnp.concatenate([e[:, 64 * half : 64 * half + 64] for e in ends], axis=1)
            own[p, half, 64 * NJ] = jnp.broadcast_to(joined.astype(BF), (2, LANES))

    def more(p):
        radial(p)
        pair_copy(p, 0).start()
        pair_copy(p, 1).start()

    def longitude(q):
        k = lax.broadcasted_iota(jnp.int32, (LANES, PLANE * 2 * PAIR_DEV), 0)
        slot = lax.broadcasted_iota(jnp.int32, (LANES, PLANE * 2 * PAIR_DEV), 1)
        picked = jnp.where(slot == (k // 2) * PAIR_DEV + q, orders_row[...].reshape(1, PLANE * 2 * PAIR_DEV).astype(F32), 0.0)
        lower = jnp.sum(picked, axis=1, keepdims=True)
        odd = lax.rem(lax.broadcasted_iota(jnp.int32, (LANES, 1), 0), 2) == 1
        order = jnp.where(odd, DEG - 1 - lower, lower)
        weight = jnp.where(order == 0, 1.0, 2.0)
        lane = lax.broadcasted_iota(jnp.int32, (LANES, LANES), 1).astype(F32)
        fine = order * lane
        cos_b, sin_b = cosine(fine, NLON), cosine(fine - NLON // 4, NLON)
        coarse = order * jnp.where(lane < NLON // LANES, lane, 0.0) * LANES
        cos_all = weight * cosine(coarse, NLON)
        sin_all = weight * cosine(coarse - NLON // 4, NLON)
        for i in range(NLON // LANES):
            cos_a, sin_a = cos_all[:, i : i + 1], sin_all[:, i : i + 1]
            cols = pl.ds(i * LANES, LANES)
            lon[pl.ds(0, 128), cols] = (cos_a * cos_b - sin_a * sin_b).astype(BF)
            lon[pl.ds(128, 128), cols] = (-(sin_a * cos_b + cos_a * sin_b)).astype(BF)

    def latitude(q, w):
        half = 1 - row if w == 0 else row
        to = 1 - plane if w == 0 else plane
        pair_copy(q, w).wait_recv()
        cut = DEG - orders[ma * PAIR_DEV + q]
        for j in range(NJ):
            piece = pl.ds(64 * j, 64)
            levels = (
                own[q, half, piece].reshape(128, LANES).astype(F32)
                + got[q, half, piece].reshape(128, LANES).astype(F32)
            )
            low = lax.broadcasted_iota(jnp.int32, (128, LANES), 1) + 128 * j < cut
            lhs[w, pl.ds(0, 128), pl.ds(128 * j, 128)] = jnp.where(low, levels, 0.0).astype(BF)
            lhs[w, pl.ds(128, 128), pl.ds(128 * j, 128)] = jnp.where(low, 0.0, levels).astype(BF)
        end = own[q, half, 64 * NJ].astype(F32) + got[q, half, 64 * NJ].astype(F32)
        end = end.astype(BF).astype(F32)[0:1]
        if w == 0:
            load_basis(q).wait()
        for b in range(5):
            cols = pl.ds(pl.multiple_of(to * 512 + 128 * b, 128), 128)
            made = lax.dot_general(
                bas[q, pl.ds(0, DEG), cols],
                lhs[w],
                (((0,), (1,)), ((), ())),
                preferred_element_type=F32,
            )
            edge = jnp.transpose(bas[q, pl.ds(DEG, 1), cols].astype(F32), (1, 0))
            mix[b % 2, pl.ds(0, 128, 2), :] = made[:, :128]
            mix[b % 2, pl.ds(1, 128, 2), :] = made[:, 128:] + edge * end
            sendbuf[q, w, pl.ds(128 * b, 128)] = mix[b % 2].astype(BF).reshape(128, 2, LANES)

    def scatter_copy(q, w, k):
        to = 1 - plane if w == 0 else plane
        other = lax.rem(place + lax.rem(k * STRIDE, PLANE), PLANE)
        return pltpu.make_async_remote_copy(
            src_ref=sendbuf.at[q, w, pl.ds(64 * to + TDEV * other, TDEV)],
            dst_ref=recvbuf.at[q, :, ma],
            send_sem=send_sem.at[q, w],
            recv_sem=recv_sem.at[q, w],
            device_id=(to * PLANE + other, 1 - row if w == 0 else row),
            device_id_type=MESH,
        )

    def scatter_across(q):
        def send(k, carry):
            scatter_copy(q, 0, k).start()
            return carry

        lax.fori_loop(0, PLANE, send, 0, unroll=4)

    def keep(q):
        return pltpu.make_async_copy(
            sendbuf.at[q, 1, pl.ds(64 * plane + TDEV * place, TDEV)],
            recvbuf.at[q, :, ma],
            recv_sem.at[q, 1],
        )

    def scatter_inside(q):
        def send(k, carry):
            scatter_copy(q, 1, k).start()
            return carry

        lax.fori_loop(1, PLANE, send, 0, unroll=4)
        keep(q).start()

    def scatter_both(q):
        scatter_copy(q, 0, 0).start()

        def send(k, carry):
            scatter_copy(q - 1, 1, k).start()
            scatter_copy(q, 0, k).start()
            return carry

        lax.fori_loop(1, PLANE, send, 0, unroll=2)
        keep(q - 1).start()

    def arrive(q):
        for w in range(2):
            arrived = recvbuf.at[q, :, pl.ds((1 - plane if w == 0 else plane) * PLANE, PLANE)]
            pltpu.make_async_copy(arrived, arrived, recv_sem.at[q, w]).wait()
        for t in range(TDEV):
            turned = recvbuf[q, t].reshape(128, LANES).T
            rx[pl.ds(64 * t, 64), pl.ds(0, 128)] = turned[:64]
            rx[pl.ds(64 * t, 64), pl.ds(128, 128)] = turned[64:]

    def receive(q, first=False):
        arrive(q)
        for g in range(3):
            part = pl.ds(384 * g, 384)
            left = rx[part, :]
            for n in range(9):
                cols = pl.ds(256 * n, 256)
                added = jnp.dot(left, lon[:, cols], preferred_element_type=F32)
                acc[part, cols] = added if first else acc[part, cols] + added

    radial(0, True)
    pl.semaphore_wait(barrier, 9)
    pair_copy(0, 0).start()
    pair_copy(0, 1).start()
    load_rows(2).start()
    for i in range(1, 4):
        signal(meet.at[0], on_y(i))
    more(1)
    load_rows(3).start()
    pl.semaphore_wait(meet.at[0], 3)
    for i in range(1, 4):
        signal(meet.at[1], on_z(i))
    more(2)
    load_rows(4).start()
    pl.semaphore_wait(meet.at[1], 3)
    signal(meet.at[2], across)
    longitude(0)
    more(3)
    load_rows(5).start()
    pl.semaphore_wait(meet.at[2], 1)
    latitude(0, 0)
    scatter_across(0)
    more(4)
    latitude(0, 1)
    latitude(1, 0)
    scatter_both(1)
    more(5)
    latitude(1, 1)
    latitude(2, 0)
    scatter_both(2)
    receive(0, True)
    longitude(1)
    latitude(2, 1)

    def step(q, carry):
        latitude(q, 0)
        scatter_both(q)

        receive(q - 2)
        longitude(q - 1)
        latitude(q, 1)
        return carry

    lax.fori_loop(3, PAIR_DEV, step, 0)

    end = PAIR_DEV - 1
    scatter_inside(end)
    receive(end - 1)
    longitude(end)
    arrive(end)

    def put(t):
        return pltpu.make_async_copy(grid.at[t], out.at[:, t], out_sem.at[t])

    for g in range(9):
        part = pl.ds(128 * g, 128)
        left = rx[part, :]
        for n in range(9):
            cols = pl.ds(256 * n, 256)
            total = (
                acc[part, cols] + jnp.dot(left, lon[:, cols], preferred_element_type=F32)
            ).astype(BF)
            for a in range(2):
                for b in range(2):
                    grid[2 * g + a, :, :, pl.ds(256 * n + 128 * b, LANES)] = total[
                        64 * a : 64 * a + 64, 128 * b : 128 * b + 128
                    ].reshape(32, 2, LANES)
        for a in range(2):
            put(2 * g + a).start()

    def drain(q, carry):
        for w in range(2):
            pair_copy(q, w).wait_send()
            sent = sendbuf.at[q, w, pl.ds(0, TDEV * (PLANE - w))]
            pltpu.make_async_copy(sent, sent, send_sem.at[q, w]).wait()
        return carry

    lax.fori_loop(0, PAIR_DEV, drain, 0)
    for t in range(TDEV):
        put(t).wait()


def write_out(grid, out, hold, read_sem, write_sem):
    reads, writes = [], []
    for i in range(8):
        piece = pl.ds(4 * i, 4)
        reads.append(pltpu.make_async_copy(grid.at[piece], hold.at[i], read_sem.at[i]))
        writes.append(pltpu.make_async_copy(hold.at[i], out.at[piece], write_sem.at[i]))
    for copy in reads:
        copy.start()
    for read, write in zip(reads, writes):
        read.wait()
        write.start()
    for copy in writes:
        copy.wait()


def per_device(spectral, latitude_basis, pair_orders):
    pair_dev, parts, local_modes, fields, packed = spectral.shape
    degrees = packed - 1
    level_dev = LEV // lax.axis_size("row")
    shape = jax.ShapeDtypeStruct((level_dev, TDEV, fields, NLON), BF)
    grid = pl.pallas_call(
        kernel,
        out_shape=shape,
        in_specs=[
            pl.BlockSpec(memory_space=pl.ANY),
            pl.BlockSpec(memory_space=pl.ANY),
            pl.BlockSpec(memory_space=pltpu.VMEM),
            pl.BlockSpec(memory_space=pltpu.SMEM),
        ],
        out_specs=pl.BlockSpec(memory_space=pl.ANY),
        scratch_shapes=[
            pltpu.VMEM((pair_dev, NJ, parts, local_modes, fields, LANES), BF),
            pltpu.VMEM((2, parts, local_modes, fields, packed), BF),
            pltpu.VMEM((pair_dev, packed, 1152), BF),
            pltpu.VMEM((pair_dev, 2, 64 * NJ + 1, 2, LANES), BF),
            pltpu.VMEM((pair_dev, 2, 64 * NJ + 1, 2, LANES), BF),
            pltpu.VMEM((2, 256, degrees), BF),
            pltpu.VMEM((pair_dev, 2, 640, 2, LANES), BF),
            pltpu.VMEM((pair_dev, TDEV, 2 * PLANE, 2, LANES), BF),
            pltpu.VMEM((256, NLON), BF),
            pltpu.VMEM((1152, 256), BF),
            pltpu.VMEM((1152, NLON), F32),
            pltpu.VMEM((2, 256, LANES), F32),
            pltpu.VMEM((LANES, fields * local_modes), BF),
            pltpu.VMEM((TDEV, level_dev, fields, NLON), BF),
            pltpu.SemaphoreType.DMA((pair_dev, NJ)),
            pltpu.SemaphoreType.DMA((2,)),
            pltpu.SemaphoreType.DMA((pair_dev,)),
            pltpu.SemaphoreType.DMA((pair_dev, 2)),
            pltpu.SemaphoreType.DMA((pair_dev, 2)),
            pltpu.SemaphoreType.DMA((pair_dev, 2)),
            pltpu.SemaphoreType.DMA((pair_dev, 2)),
            pltpu.SemaphoreType.REGULAR((3,)),
            pltpu.SemaphoreType.DMA((TDEV,)),
        ],
        compiler_params=pltpu.CompilerParams(
            collective_id=0, has_side_effects=True, vmem_limit_bytes=60 * 2**20
        ),
    )(spectral, latitude_basis, pair_orders, pair_orders)
    result = pl.pallas_call(
        write_out,
        out_shape=shape,
        in_specs=[pl.BlockSpec(memory_space=pl.ANY)],
        out_specs=pl.BlockSpec(memory_space=pl.ANY),
        scratch_shapes=[
            pltpu.VMEM((8, level_dev // 8, TDEV, fields, NLON), BF),
            pltpu.SemaphoreType.DMA((8,)),
            pltpu.SemaphoreType.DMA((8,)),
        ],
        compiler_params=pltpu.CompilerParams(vmem_limit_bytes=63 * 2**20),
    )(grid)
    return jnp.transpose(result, (0, 2, 1, 3))


def solution(mesh):
    return jax.shard_map(
        per_device,
        mesh=mesh,
        in_specs=(P("ma", None, "row", None, None), P("ma", None, None), P()),
        out_specs=P("row", None, "ma", None),
        check_vma=False,
    )
```

```python
import functools
import math

import jax
import jax.numpy as jnp
from jax import lax
from jax.experimental import pallas as pl
from jax.experimental.pallas import tpu as pltpu
from jax.sharding import PartitionSpec as P

NLON = 2304
LEV = 64
MESH = pl.DeviceIdType.MESH
BF = jnp.bfloat16
F32 = jnp.float32

PLANE = 32
STRIDE = 11
PAIR_DEV = 6
LANES = 128
TDEV = 18
NJ = 6
DEG = 768
MODES = 192
TURN = 2.0 * math.pi


def cosine(steps, period):
    left = steps - period * jnp.floor(steps * (1.0 / period) + 0.5)
    size = jnp.abs(left)
    flip = size > period / 4
    angle = jnp.where(flip, period / 2 - size, size) * (TURN / period)
    square = angle * angle
    total = jnp.full_like(square, -1.0 / math.factorial(14))
    for n in range(12, -1, -2):
        total = total * square + (-1.0) ** (n // 2) / math.factorial(n)
    return jnp.where(flip, -total, total)


def kernel(
    spec, basis, orders_row, orders, out,
    stage, rows, bas, own, got, lhs, sendbuf, recvbuf, lon, rx, acc, mix, table, grid,
    spec_sem, rows_sem, bas_sem, pair_send, pair_recv, send_sem, recv_sem, meet, out_sem,
):
    ma = lax.axis_index("ma")
    row = lax.axis_index("row")
    plane = ma // PLANE
    place = lax.rem(ma, PLANE)
    along_y, along_z, core = place // 8, lax.rem(place // 2, 4), lax.rem(place, 2)

    def load_spec(p, j):
        return pltpu.make_async_copy(
            spec.at[p, :, :, :, pl.ds(j * LANES, LANES)], stage.at[p, j], spec_sem.at[p, j]
        )

    def load_rows(p):
        slot = lax.rem(p, 2)
        return pltpu.make_async_copy(spec.at[p], rows.at[slot], rows_sem.at[slot])

    def load_basis(p):
        return pltpu.make_async_copy(basis.at[p], bas.at[p], bas_sem.at[p])

    for j in range(NJ):
        load_spec(0, j).start()
    load_rows(0).start()

    def load_others():
        for p in range(1, PAIR_DEV):
            for j in range(NJ):
                load_spec(p, j).start()
            if p == 1:
                load_rows(1).start()
            else:
                load_basis(p - 2).start()
        for p in range(PAIR_DEV - 2, PAIR_DEV):
            load_basis(p).start()

    def signal(sem, device):
        pl.semaphore_signal(sem, inc=1, device_id=device, device_id_type=MESH)

    def on_y(i):
        return plane * PLANE + lax.rem(along_y + i, 4) * 8 + along_z * 2 + core, row

    def on_z(i):
        return plane * PLANE + along_y * 8 + lax.rem(along_z + i, 4) * 2 + core, row

    across = ((1 - plane) * PLANE + place, 1 - row)
    barrier = pltpu.get_barrier_semaphore()
    signal(barrier, (ma, 1 - row))
    for i in range(1, 4):
        signal(barrier, on_y(i))
    for i in range(1, 4):
        signal(barrier, on_z(i))
    signal(barrier, (plane * PLANE + along_y * 8 + along_z * 2 + 1 - core, row))
    signal(barrier, across)

    level = lax.broadcasted_iota(jnp.int32, (LANES, 2 * MODES), 0)
    mode = lax.broadcasted_iota(jnp.int32, (LANES, 2 * MODES), 1)
    steps = (level // 2) * (mode // 2 + row * MODES)
    same = lax.rem(level, 2) == lax.rem(mode, 2)
    period = 2 * (2 * MODES - 1)
    table[...] = jnp.where(same, cosine(steps.astype(F32), period), 0.0).astype(BF)

    def pair_copy(p, w):
        half = row if w == 0 else 1 - row
        return pltpu.make_async_remote_copy(
            src_ref=own.at[p, half],
            dst_ref=got.at[p, half],
            send_sem=pair_send.at[p, w],
            recv_sem=pair_recv.at[p, w],
            device_id=(ma, 1 - row),
            device_id_type=MESH,
        )

    def radial(p, first=False):
        ends = []
        for j in range(NJ):
            load_spec(p, j).wait()
            if first and j == NJ - 1:
                load_others()
            for c in range(2):
                modes = stage[p, j, c].reshape(2 * MODES, LANES)
                part = jnp.dot(table[...], modes, preferred_element_type=F32).astype(BF)
                for half in range(2):
                    own[p, half, pl.ds(64 * j + 32 * c, 32)] = part[
                        64 * half : 64 * half + 64
                    ].reshape(32, 2, LANES)
        load_rows(p).wait()
        for c in range(2):
            modes = rows[lax.rem(p, 2), c, :, :, DEG : DEG + 1].reshape(2 * MODES, 1)
            ends.append(
                lax.dot_general(
                    modes, table[...], (((0,), (1,)), ((), ())), preferred_element_type=F32
                )
            )
        for half in range(2):
            joined = jnp.concatenate([e[:, 64 * half : 64 * half + 64] for e in ends], axis=1)
            own[p, half, 64 * NJ] = jnp.broadcast_to(joined.astype(BF), (2, LANES))

    def more(p):
        radial(p)
        pair_copy(p, 0).start()
        pair_copy(p, 1).start()

    def longitude(q):
        k = lax.broadcasted_iota(jnp.int32, (LANES, PLANE * 2 * PAIR_DEV), 0)
        slot = lax.broadcasted_iota(jnp.int32, (LANES, PLANE * 2 * PAIR_DEV), 1)
        picked = jnp.where(slot == (k // 2) * PAIR_DEV + q, orders_row[...].reshape(1, PLANE * 2 * PAIR_DEV).astype(F32), 0.0)
        lower = jnp.sum(picked, axis=1, keepdims=True)
        odd = lax.rem(lax.broadcasted_iota(jnp.int32, (LANES, 1), 0), 2) == 1
        order = jnp.where(odd, DEG - 1 - lower, lower)
        weight = jnp.where(order == 0, 1.0, 2.0)
        lane = lax.broadcasted_iota(jnp.int32, (LANES, LANES), 1).astype(F32)
        fine = order * lane
        cos_b, sin_b = cosine(fine, NLON), cosine(fine - NLON // 4, NLON)
        coarse = order * jnp.where(lane < NLON // LANES, lane, 0.0) * LANES
        cos_all = weight * cosine(coarse, NLON)
        sin_all = weight * cosine(coarse - NLON // 4, NLON)
        for i in range(NLON // LANES):
            cos_a, sin_a = cos_all[:, i : i + 1], sin_all[:, i : i + 1]
            cols = pl.ds(i * LANES, LANES)
            lon[pl.ds(0, 128), cols] = (cos_a * cos_b - sin_a * sin_b).astype(BF)
            lon[pl.ds(128, 128), cols] = (-(sin_a * cos_b + cos_a * sin_b)).astype(BF)

    def latitude(q, w):
        half = 1 - row if w == 0 else row
        to = 1 - plane if w == 0 else plane
        pair_copy(q, w).wait_recv()
        cut = DEG - orders[ma * PAIR_DEV + q]
        for j in range(NJ):
            piece = pl.ds(64 * j, 64)
            levels = (
                own[q, half, piece].reshape(128, LANES).astype(F32)
                + got[q, half, piece].reshape(128, LANES).astype(F32)
            )
            low = lax.broadcasted_iota(jnp.int32, (128, LANES), 1) + 128 * j < cut
            lhs[w, pl.ds(0, 128), pl.ds(128 * j, 128)] = jnp.where(low, levels, 0.0).astype(BF)
            lhs[w, pl.ds(128, 128), pl.ds(128 * j, 128)] = jnp.where(low, 0.0, levels).astype(BF)
        end = own[q, half, 64 * NJ].astype(F32) + got[q, half, 64 * NJ].astype(F32)
        end = end.astype(BF).astype(F32)[0:1]
        if w == 0:
            load_basis(q).wait()
        for b in range(5):
            cols = pl.ds(pl.multiple_of(to * 512 + 128 * b, 128), 128)
            made = lax.dot_general(
                bas[q, pl.ds(0, DEG), cols],
                lhs[w],
                (((0,), (1,)), ((), ())),
                preferred_element_type=F32,
            )
            edge = jnp.transpose(bas[q, pl.ds(DEG, 1), cols].astype(F32), (1, 0))
            mix[b % 2, pl.ds(0, 128, 2), :] = made[:, :128]
            mix[b % 2, pl.ds(1, 128, 2), :] = made[:, 128:] + edge * end
            sendbuf[q, w, pl.ds(128 * b, 128)] = mix[b % 2].astype(BF).reshape(128, 2, LANES)

    def scatter_copy(q, w, k):
        to = 1 - plane if w == 0 else plane
        other = lax.rem(place + lax.rem(k * STRIDE, PLANE), PLANE)
        return pltpu.make_async_remote_copy(
            src_ref=sendbuf.at[q, w, pl.ds(64 * to + TDEV * other, TDEV)],
            dst_ref=recvbuf.at[q, :, ma],
            send_sem=send_sem.at[q, w],
            recv_sem=recv_sem.at[q, w],
            device_id=(to * PLANE + other, 1 - row if w == 0 else row),
            device_id_type=MESH,
        )

    def scatter_across(q):
        def send(k, carry):
            scatter_copy(q, 0, k).start()
            return carry

        lax.fori_loop(0, PLANE, send, 0, unroll=4)

    def keep(q):
        return pltpu.make_async_copy(
            sendbuf.at[q, 1, pl.ds(64 * plane + TDEV * place, TDEV)],
            recvbuf.at[q, :, ma],
            recv_sem.at[q, 1],
        )

    def scatter_inside(q):
        def send(k, carry):
            scatter_copy(q, 1, k).start()
            return carry

        lax.fori_loop(1, PLANE, send, 0, unroll=4)
        keep(q).start()

    def scatter_both(q):
        scatter_copy(q, 0, 0).start()

        def send(k, carry):
            scatter_copy(q - 1, 1, k).start()
            scatter_copy(q, 0, k).start()
            return carry

        lax.fori_loop(1, PLANE, send, 0, unroll=2)
        keep(q - 1).start()

    def arrive(q):
        for w in range(2):
            arrived = recvbuf.at[q, :, pl.ds((1 - plane if w == 0 else plane) * PLANE, PLANE)]
            pltpu.make_async_copy(arrived, arrived, recv_sem.at[q, w]).wait()
        for t in range(TDEV):
            turned = recvbuf[q, t].reshape(128, LANES).T
            rx[pl.ds(64 * t, 64), pl.ds(0, 128)] = turned[:64]
            rx[pl.ds(64 * t, 64), pl.ds(128, 128)] = turned[64:]

    def receive(q, first=False):
        arrive(q)
        for g in range(3):
            part = pl.ds(384 * g, 384)
            left = rx[part, :]
            for n in range(9):
                cols = pl.ds(256 * n, 256)
                added = jnp.dot(left, lon[:, cols], preferred_element_type=F32)
                acc[part, cols] = added if first else acc[part, cols] + added

    radial(0, True)
    pl.semaphore_wait(barrier, 9)
    pair_copy(0, 0).start()
    pair_copy(0, 1).start()
    load_rows(2).start()
    for i in range(1, 4):
        signal(meet.at[0], on_y(i))
    more(1)
    load_rows(3).start()
    pl.semaphore_wait(meet.at[0], 3)
    for i in range(1, 4):
        signal(meet.at[1], on_z(i))
    more(2)
    load_rows(4).start()
    pl.semaphore_wait(meet.at[1], 3)
    signal(meet.at[2], across)
    longitude(0)
    more(3)
    load_rows(5).start()
    pl.semaphore_wait(meet.at[2], 1)
    latitude(0, 0)
    scatter_across(0)
    more(4)
    latitude(0, 1)
    latitude(1, 0)
    scatter_both(1)
    more(5)
    latitude(1, 1)
    latitude(2, 0)
    scatter_both(2)
    receive(0, True)
    longitude(1)
    latitude(2, 1)

    def step(q, carry):
        latitude(q, 0)
        scatter_both(q)

        receive(q - 2)
        longitude(q - 1)
        latitude(q, 1)
        return carry

    lax.fori_loop(3, PAIR_DEV, step, 0)

    end = PAIR_DEV - 1
    scatter_inside(end)
    receive(end - 1)
    longitude(end)
    arrive(end)

    def put(t):
        return pltpu.make_async_copy(grid.at[t], out.at[:, t], out_sem.at[t])

    for g in range(9):
        part = pl.ds(128 * g, 128)
        left = rx[part, :]
        for n in range(9):
            cols = pl.ds(256 * n, 256)
            total = (
                acc[part, cols] + jnp.dot(left, lon[:, cols], preferred_element_type=F32)
            ).astype(BF)
            for a in range(2):
                for b in range(2):
                    grid[2 * g + a, :, :, pl.ds(256 * n + 128 * b, LANES)] = total[
                        64 * a : 64 * a + 64, 128 * b : 128 * b + 128
                    ].reshape(32, 2, LANES)
        for a in range(2):
            put(2 * g + a).start()

    def drain(q, carry):
        for w in range(2):
            pair_copy(q, w).wait_send()
            sent = sendbuf.at[q, w, pl.ds(0, TDEV * (PLANE - w))]
            pltpu.make_async_copy(sent, sent, send_sem.at[q, w]).wait()
        return carry

    lax.fori_loop(0, PAIR_DEV, drain, 0)
    for t in range(TDEV):
        put(t).wait()


def write_out(grid, out, hold, read_sem, write_sem):
    reads, writes = [], []
    for i in range(4):
        piece = pl.ds(8 * i, 8)
        reads.append(pltpu.make_async_copy(grid.at[piece], hold.at[i], read_sem.at[i]))
        writes.append(pltpu.make_async_copy(hold.at[i], out.at[piece], write_sem.at[i]))
    for copy in reads:
        copy.start()
    for read, write in zip(reads, writes):
        read.wait()
        write.start()
    for copy in writes:
        copy.wait()


def per_device(spectral, latitude_basis, pair_orders):
    pair_dev, parts, local_modes, fields, packed = spectral.shape
    degrees = packed - 1
    level_dev = LEV // lax.axis_size("row")
    shape = jax.ShapeDtypeStruct((level_dev, TDEV, fields, NLON), BF)
    grid = pl.pallas_call(
        kernel,
        out_shape=shape,
        in_specs=[
            pl.BlockSpec(memory_space=pl.ANY),
            pl.BlockSpec(memory_space=pl.ANY),
            pl.BlockSpec(memory_space=pltpu.VMEM),
            pl.BlockSpec(memory_space=pltpu.SMEM),
        ],
        out_specs=pl.BlockSpec(memory_space=pl.ANY),
        scratch_shapes=[
            pltpu.VMEM((pair_dev, NJ, parts, local_modes, fields, LANES), BF),
            pltpu.VMEM((2, parts, local_modes, fields, packed), BF),
            pltpu.VMEM((pair_dev, packed, 1152), BF),
            pltpu.VMEM((pair_dev, 2, 64 * NJ + 1, 2, LANES), BF),
            pltpu.VMEM((pair_dev, 2, 64 * NJ + 1, 2, LANES), BF),
            pltpu.VMEM((2, 256, degrees), BF),
            pltpu.VMEM((pair_dev, 2, 640, 2, LANES), BF),
            pltpu.VMEM((pair_dev, TDEV, 2 * PLANE, 2, LANES), BF),
            pltpu.VMEM((256, NLON), BF),
            pltpu.VMEM((1152, 256), BF),
            pltpu.VMEM((1152, NLON), F32),
            pltpu.VMEM((2, 256, LANES), F32),
            pltpu.VMEM((LANES, fields * local_modes), BF),
            pltpu.VMEM((TDEV, level_dev, fields, NLON), BF),
            pltpu.SemaphoreType.DMA((pair_dev, NJ)),
            pltpu.SemaphoreType.DMA((2,)),
            pltpu.SemaphoreType.DMA((pair_dev,)),
            pltpu.SemaphoreType.DMA((pair_dev, 2)),
            pltpu.SemaphoreType.DMA((pair_dev, 2)),
            pltpu.SemaphoreType.DMA((pair_dev, 2)),
            pltpu.SemaphoreType.DMA((pair_dev, 2)),
            pltpu.SemaphoreType.REGULAR((3,)),
            pltpu.SemaphoreType.DMA((TDEV,)),
        ],
        compiler_params=pltpu.CompilerParams(
            collective_id=0, has_side_effects=True, vmem_limit_bytes=60 * 2**20
        ),
    )(spectral, latitude_basis, pair_orders, pair_orders)
    result = pl.pallas_call(
        write_out,
        out_shape=shape,
        in_specs=[pl.BlockSpec(memory_space=pl.ANY)],
        out_specs=pl.BlockSpec(memory_space=pl.ANY),
        scratch_shapes=[
            pltpu.VMEM((4, level_dev // 4, TDEV, fields, NLON), BF),
            pltpu.SemaphoreType.DMA((4,)),
            pltpu.SemaphoreType.DMA((4,)),
        ],
        compiler_params=pltpu.CompilerParams(vmem_limit_bytes=63 * 2**20),
    )(grid)
    return jnp.transpose(result, (0, 2, 1, 3))


def solution(mesh):
    return jax.shard_map(
        per_device,
        mesh=mesh,
        in_specs=(P("ma", None, "row", None, None), P("ma", None, None), P()),
        out_specs=P("row", None, "ma", None),
        check_vma=False,
    )
```
